32 devices in a mesh: row: 8 (over y, x, core), col: 4 (over z).
Axes of the slice: x: 2, y: 2, z: 4, core: 2. Of those that a mesh axis runs over, the one named last changes fastest.
Arguments:
- source: float32 [512, 512, 512], P('row', 'col'), may hold values from -8 to 8
- basis_x: float32 [512, 512], replicated, may hold values from -0.25 to 0.25
- basis_y: float32 [512, 512], replicated, may hold values from -0.25 to 0.25
- basis_z: float32 [512, 512], replicated, may hold values from -0.25 to 0.25
- eigen_x: float32 [512], replicated, may hold values from 0.1 to 10
- eigen_y: float32 [512], replicated, may hold values from 0.1 to 10
- eigen_z: float32 [512], replicated, may hold values from 0.1 to 10
Outputs:
- solution: float32 [512, 512, 512], P('row', 'col')
The draws below stay inside these ranges and needn't reach their ends.
All inputs are finite; a program needn't handle non-finite values.
Results may differ from the reference program's by a relative error of at most 0.00007.
Values sent between devices are 32-bit elements; how exact they have to be, the bound alone decides.
A program may use at most 128 MiB of HBM per device.

```python
import math
import jax
import jax.numpy as jnp
from jax import lax

NX = 512
NY = 512
NZ = 512


def levels(stream_key, extent, cuts, smallest, top_value):
    level, own = 1.0, jax.random.fold_in(stream_key, 6)
    for axis_at, parts in cuts:
        draws = jnp.exp(jax.random.uniform(jax.random.fold_in(own, axis_at), (parts,), jnp.float32, smallest / len(cuts), top_value / len(cuts)))
        level = level * jnp.repeat(draws, extent[axis_at] // parts).reshape([-1 if axis == axis_at else 1 for axis in range(len(extent))])
    return level


def gaussian(stream_key, extent, width, limit, split=(), held_as=jnp.bfloat16):
    values = jax.random.normal(stream_key, extent, jnp.float32) * width
    if len(split) > 0:
        values = levels(stream_key, extent, split, -0.22, 0.18) * values
    return jnp.clip(values, min=-limit, max=limit).astype(held_as)


def setup_inputs(seed: int = 0) -> dict:
    keys = jax.random.split(jax.random.key(seed), 8)
    source = gaussian(keys[0], (NX, NY, NZ), 1.0, 8.0, ((0, 8), (1, 4)), jnp.float32)
    basis_x = gaussian(keys[1], (NX, NX), NX ** -0.5, 0.25, (), jnp.float32)
    basis_y = gaussian(keys[2], (NY, NY), NY ** -0.5, 0.25, (), jnp.float32)
    basis_z = gaussian(keys[3], (NZ, NZ), NZ ** -0.5, 0.25, (), jnp.float32)
    eigen_x = jnp.clip(jnp.exp(jax.random.uniform(keys[4], (NX,), jnp.float32, math.log(0.1), math.log(10.0))), 0.1, 10.0)
    eigen_y = jnp.clip(jnp.exp(jax.random.uniform(keys[5], (NY,), jnp.float32, math.log(0.1), math.log(10.0))), 0.1, 10.0)
    eigen_z = jnp.clip(jnp.exp(jax.random.uniform(keys[6], (NZ,), jnp.float32, math.log(0.1), math.log(10.0))), 0.1, 10.0)
    return {"source": source, "basis_x": basis_x, "basis_y": basis_y, "basis_z": basis_z, "eigen_x": eigen_x, "eigen_y": eigen_y, "eigen_z": eigen_z}


HIGH = lax.Precision.HIGHEST


def reference(source, basis_x, basis_y, basis_z, eigen_x, eigen_y, eigen_z):
    field = jnp.einsum('ai,abc->ibc', basis_x, source, precision=HIGH)
    field = jnp.einsum('bj,ibc->ijc', basis_y, field, precision=HIGH)
    field = jnp.einsum('ck,ijc->ijk', basis_z, field, precision=HIGH)
    denom = eigen_x[:, None, None] + eigen_y[None, :, None] + eigen_z[None, None, :]
    field = field / denom
    field = jnp.einsum('ck,ijk->ijc', basis_z, field, precision=HIGH)
    field = jnp.einsum('bj,ijc->ibc', basis_y, field, precision=HIGH)
    field = jnp.einsum('ai,ibc->abc', basis_x, field, precision=HIGH)
    return field
```

```python
import math

import jax
import jax.numpy as jnp
from jax import lax
from jax.sharding import PartitionSpec as P

PREC = lax.Precision.HIGH
CHUNKS = 4


def local(source, basis_x, basis_y, basis_z, eigen_x, eigen_y, eigen_z):
    rows_n = lax.axis_size("row")
    cols_n = lax.axis_size("col")
    devices = rows_n * cols_n
    me = lax.axis_index("row") * cols_n + lax.axis_index("col")
    ax, by, nz = source.shape
    nx, ny = basis_x.shape[0], basis_y.shape[0]
    planes = nz // devices
    chunks = math.gcd(CHUNKS, planes)
    step = planes // chunks
    bz = basis_z.reshape(nz, devices, chunks, step)
    ez = lax.dynamic_slice_in_dim(eigen_z, me * planes, planes, 0).reshape(chunks, step)
    exy = eigen_x[:, None] + eigen_y[None, :]

    def forward(c):
        part = bz[:, :, c, :].reshape(nz, devices * step)
        field = jnp.einsum("ck,abc->kab", part, source, precision=PREC)
        return lax.all_to_all(field, ("row", "col"), split_axis=0, concat_axis=0, tiled=True)

    def middle(c, field):
        field = field.reshape(rows_n, cols_n, step, ax, by)
        field = field.transpose(2, 0, 3, 1, 4).reshape(step, nx, ny)
        field = jnp.einsum("xi,kxy->kiy", basis_x, field, precision=PREC)
        field = jnp.einsum("kiy,yj->kij", field, basis_y, precision=PREC)
        field = field / (exy[None] + ez[c][:, None, None])
        field = jnp.einsum("kij,yj->kiy", field, basis_y, precision=PREC)
        field = jnp.einsum("xi,kiy->kxy", basis_x, field, precision=PREC)
        field = field.reshape(step, rows_n, ax, cols_n, by).transpose(1, 3, 0, 2, 4)
        field = field.reshape(devices * step, ax, by)
        return lax.all_to_all(field, ("row", "col"), split_axis=0, concat_axis=0, tiled=True)

    def backward(c, field):
        part = bz[:, :, c, :].reshape(nz, devices * step)
        return jnp.einsum("ck,kab->abc", part, field, precision=PREC)

    arrived = [forward(c) for c in range(chunks)]
    returned = [middle(c, arrived[c]) for c in range(chunks)]
    out = backward(0, returned[0])
    for c in range(1, chunks):
        out = out + backward(c, returned[c])
    return out


def solution(mesh):
    placed = (P("row", "col", None), P(), P(), P(), P(), P(), P())
    return jax.shard_map(
        local, mesh=mesh, in_specs=placed, out_specs=P("row", "col", None), check_vma=False
    )
```

```python
import jax
import jax.numpy as jnp
from jax import lax
from jax.experimental.layout import Layout, with_layout_constraint
from jax.sharding import PartitionSpec as P

FAST = lax.Precision.HIGH
FULL = lax.Precision.HIGHEST


def cuts(planes):
    if planes < 3:
        return [(p, 1) for p in range(planes)]
    first = max(1, planes * 2 // 16)
    last = max(1, planes * 6 // 16)
    return [(0, first), (first, planes - first - last), (planes - last, last)]


def local(source, basis_x, basis_y, basis_z, eigen_x, eigen_y, eigen_z):
    rows_n = lax.axis_size("row")
    cols_n = lax.axis_size("col")
    devices = rows_n * cols_n
    me = lax.axis_index("row") * cols_n + lax.axis_index("col")
    ax, by, nz = source.shape
    nx, ny = basis_x.shape[0], basis_y.shape[0]
    planes = nz // devices
    bz = basis_z.reshape(nz, devices, planes)
    ez = lax.dynamic_slice_in_dim(eigen_z, me * planes, planes, 0)
    exy = eigen_x[:, None] + eigen_y[None, :]
    pieces = cuts(planes)

    def columns(piece):
        start, count = piece
        return bz[:, :, start : start + count].reshape(nz, devices * count)

    def exchange(field):
        return lax.all_to_all(field, ("row", "col"), split_axis=0, concat_axis=0, tiled=True)

    def forward(piece):
        field = jnp.einsum("ck,abc->kab", columns(piece), source, precision=FAST)
        return with_layout_constraint(field, Layout(major_to_minor=(0, 1, 2)))

    def middle(piece, field):
        start, count = piece
        field = field.reshape(rows_n, cols_n, count, ax, by)
        field = field.transpose(2, 0, 3, 1, 4).reshape(count, nx, ny)
        field = jnp.einsum("xi,kxy->kiy", basis_x, field, precision=FULL)
        field = jnp.einsum("kiy,yj->kij", field, basis_y, precision=FULL)
        field = field / (exy[None] + ez[start : start + count][:, None, None])
        field = jnp.einsum("kij,yj->kiy", field, basis_y, precision=FULL)
        field = jnp.einsum("xi,kiy->kxy", basis_x, field, precision=FULL)
        field = field.reshape(count, rows_n, ax, cols_n, by).transpose(1, 3, 0, 2, 4)
        return field.reshape(devices * count, ax, by)

    def backward(piece, field, precision):
        return jnp.einsum("ck,kab->abc", columns(piece), field, precision=precision)

    count = len(pieces)
    tie = lax.optimization_barrier
    fields = [forward(pieces[0])]
    arrived = [exchange(fields[0])]
    done = []
    for n in range(1, count):
        field = forward(pieces[n])
        if done:
            arrived[-1], field, done[-1] = tie((arrived[-1], field, done[-1]))
        else:
            arrived[-1], field = tie((arrived[-1], field))
        arrived.append(exchange(field))
        done.append(middle(pieces[n - 1], arrived[n - 1]))
    if done:
        arrived[-1], *done = tie((arrived[-1], *done))
    returned = []
    for n, piece in enumerate(pieces):
        if n == count - 1:
            if count > 2:
                returned[0], arrived[-1] = tie((returned[0], arrived[-1]))
            done.append(middle(piece, arrived[-1]))
        field = done[n]
        if returned:
            returned[-1], field = tie((returned[-1], field))
        returned.append(exchange(field))
    total = backward(pieces[0], returned[0], FULL)
    for piece, field in zip(pieces[1:], returned[1:]):
        total = lax.optimization_barrier(total)
        last = piece is pieces[-1]
        total = total + backward(piece, field, FAST if last else FULL)
    return total


def solution(mesh):
    placed = (P("row", "col", None), P(), P(), P(), P(), P(), P())
    return jax.shard_map(
        local, mesh=mesh, in_specs=placed, out_specs=P("row", "col", None), check_vma=False
    )
```
